32 devices in a mesh: gx: 4 (over x, core), gy: 8 (over z, y).
Axes of the slice: x: 2, y: 2, z: 4, core: 2. Of those that a mesh axis runs over, the one named last changes fastest.
Arguments:
- hot_ids: int32 [262144], P(('gx', 'gy')), may hold values from 0 to 2047
- hot_grads: bfloat16 [262144, 128], P(('gx', 'gy')), may hold values from -6 to 6
- cold_grads: bfloat16 [4, 8, 8, 512, 128], P('gx', 'gy'), may hold values from -6 to 6
- cold_slots: int32 [4, 8, 8, 512], P('gx', 'gy'), may hold values from 0 to 2047
- cold_counts: int32 [4, 8, 8], P('gx', 'gy'), may hold values from 1 to 512, as said below
Outputs:
- hot_grad: float32 [2048, 128], replicated
- cold_grad: float32 [4, 16384, 128], P('gx', 'gy')
The draws below stay inside these ranges and needn't reach their ends.
Inputs may be any that keep to these rules, and one draw needn't show every extreme that they name: In each group g, some owner d receives cold_counts[g, s, d] = 512 from every s; loads per owner are skewed.
All inputs are finite; a program needn't handle non-finite values.
Results may differ from the reference program's by a relative error of at most 0.0003.
Values may be sent and summed in bfloat16 or wider, within the bound.
A program may use at most 64 MiB of HBM per device.

```python
import jax
import jax.numpy as jnp
from jax import lax

D = 128
HOT = 2048
LOOK = 8192
CAP = 512
OWN_ROWS = 2048
LOOKUPS = 262144
N_GX = 4
N_GY = 8


def draw_cold_counts(key, part):
    first = jax.random.fold_in(key, 11)
    second = jax.random.fold_in(key, 12)
    third = jax.random.fold_in(key, 13)
    limits = jax.random.randint(first, (N_GX, 1, N_GY), 1, CAP + 1)
    counts = jax.random.randint(second, (N_GX, N_GY, N_GY), 1, CAP + 1)
    counts = jnp.minimum(counts, limits)
    heavy = jax.random.randint(third, (N_GX, 1, 1), 0, N_GY)
    owners = jnp.arange(N_GY, dtype=jnp.int32)[None, None, :]
    return jnp.where(owners == heavy, CAP, counts).astype(jnp.int32)


def with_ends(values, rng, least, high):
    dims = values.shape
    spot = [jax.random.randint(jax.random.fold_in(rng, axis), (), 0, dims[axis]) for axis in range(len(dims))]
    values = values.at[tuple(spot)].set(least)
    longest = dims.index(max(dims))
    spot[longest] = (spot[longest] + 1) % dims[longest]
    return values.at[tuple(spot)].set(high)


def block_levels(rng, dims, shards, low, top_value):
    def one(dim, blocks):
        steps = jax.random.uniform(jax.random.fold_in(jax.random.fold_in(rng, 6), dim), (blocks,), jnp.float32, low / len(shards), top_value / len(shards))
        return jnp.repeat(jnp.exp(steps), dims[dim] // blocks).reshape((-1,) + (1,) * (len(dims) - dim - 1))

    gain = one(*shards[0])
    for cut in shards[1:]:
        gain = gain * one(*cut)
    return gain


def scatter_about(own_key, shape, spread, bound, split=(), kind=jnp.bfloat16):
    gain = block_levels(own_key, shape, split, -0.22, 0.18) if split else 1.0
    result = jax.random.normal(own_key, shape, jnp.float32) * spread * gain
    return jnp.minimum(jnp.maximum(result, -bound), bound).astype(kind)


def setup_inputs(seed: int = 0) -> dict:
    arg_keys = jax.random.split(jax.random.key(seed), 6)
    hot_ids = with_ends(jax.random.randint(arg_keys[0], (LOOKUPS,), 0, HOT), jax.random.fold_in(arg_keys[0], 1), 0, HOT - 1).astype(jnp.int32)
    hot_grads = scatter_about(arg_keys[1], (LOOKUPS, D), 1.0, 6.0, ((0, 32),))
    cold_grads = scatter_about(arg_keys[2], (N_GX, N_GY, N_GY, CAP, D), 1.0, 6.0, ((0, 4), (1, 8)))
    cold_slots = with_ends(jax.random.randint(arg_keys[3], (N_GX, N_GY, N_GY, CAP), 0, OWN_ROWS), jax.random.fold_in(arg_keys[3], 1), 0, OWN_ROWS - 1).astype(jnp.int32)
    cold_counts = draw_cold_counts(jax.random.fold_in(arg_keys[5], 71), 0)
    return dict(hot_ids=hot_ids, hot_grads=hot_grads, cold_grads=cold_grads, cold_slots=cold_slots, cold_counts=cold_counts)


def reference(hot_ids, hot_grads, cold_grads, cold_slots, cold_counts):
    hot_sum = jax.ops.segment_sum(hot_grads.astype(jnp.float32), hot_ids, num_segments=HOT)
    hot_grad = hot_sum * (HOT / (LOOK * N_GX * N_GY)) ** 0.5
    places = jnp.arange(CAP, dtype=jnp.int32)
    valid = places[None, None, None, :] < cold_counts[..., None]
    payload = jnp.where(valid[..., None], cold_grads, jnp.zeros_like(cold_grads))
    owners = jnp.arange(N_GY, dtype=jnp.int32)[None, None, :, None] * OWN_ROWS
    table_rows = (owners + cold_slots).astype(jnp.int32)

    def one_group(pair):
        rows_data, rows_index = pair
        return jax.ops.segment_sum(rows_data.reshape(-1, D).astype(jnp.float32), rows_index.reshape(-1), num_segments=OWN_ROWS * N_GY)

    cold_grad = lax.map(one_group, (payload, table_rows))
    return hot_grad, cold_grad
```

```python
import functools

import jax
import jax.numpy as jnp
from jax import lax
from jax.experimental import pallas as pl
from jax.experimental.pallas import tpu as pltpu
from jax.sharding import PartitionSpec as P

HOT = 2048
OWN_ROWS = 2048
LANES = 128
HIGH = 4
KBLOCK = 4096
MESH = pl.DeviceIdType.MESH
bf16, f32, i16 = jnp.bfloat16, jnp.float32, jnp.int16


def bits(n):
    assert n & (n - 1) == 0
    return n.bit_length() - 1


def one_hot(row, size):
    places = lax.broadcasted_iota(jnp.int32, (size, LANES), 0).astype(i16)
    return jnp.where(places == jnp.concatenate([row] * (size // 16), axis=0), bf16(1), bf16(0))


def spread(codes, data, wanted):
    return jnp.concatenate(
        [jnp.where(codes == i16(w), data, jnp.zeros_like(data)) for w in wanted], axis=1
    )


def kernel(
    nx, ny, factor, waves,
    ids_ref, hot_ref, slots_ref, counts_ref, cold_ref, hot_out, cold_out,
    hotv, idsv, codes, lows, slotv, sstage, crecv, srecv, tab, mine, give, take,
    l1a, l1b, l2a, l2b, l3a, l3b,
    local_sem, csend, crsem, ssend, srsem, hsend, hrecv,
):
    gx, gy = lax.axis_index("gx"), lax.axis_index("gy")
    px, py = 2, 2
    nxr, nyr = nx // px, ny // py
    cc, xx = lax.rem(gx, px), gx // px
    yy, zz = lax.rem(gy, py), gy // py
    piece = HOT // (2 * nx * ny)
    chain = HOT // px // 2
    half = chain // 2
    kblocks = hotv.shape[0] // KBLOCK
    cap_pieces = crecv.shape[1] // LANES
    own_low = OWN_ROWS // HIGH

    def at(c, x, y, z):
        return (x * px + c, z * py + y)

    def near_x(j):
        return at(cc, lax.rem(xx + j, nxr), yy, zz)

    def near_y(j):
        return at(cc, xx, lax.rem(yy + j, py), zz)

    def near_z(j):
        return at(cc, xx, yy, lax.rem(zz + j, nyr))

    def plane(dx, dy):
        return at(cc, lax.rem(xx + dx, nxr), lax.rem(yy + dy, py), zz)

    partner = at(1 - cc, xx, yy, zz)

    def cold_peer(t, sign):
        da, db = t // py, t % py
        a = lax.rem(zz + sign * da + nyr, nyr)
        b = lax.rem(yy + sign * db + py, py)
        return a * py + b

    ids_copy = pltpu.make_async_copy(ids_ref, idsv, local_sem.at[0])
    slots_copy = pltpu.make_async_copy(slots_ref, slotv, local_sem.at[1])
    own_copy = pltpu.make_async_copy(cold_ref.at[gy], crecv.at[0], local_sem.at[2])
    hot_copies = [
        pltpu.make_async_copy(
            hot_ref.at[pl.ds(k * KBLOCK, KBLOCK), :], hotv.at[pl.ds(k * KBLOCK, KBLOCK), :], local_sem.at[3 + k]
        )
        for k in range(kblocks)
    ]
    barrier = pltpu.get_barrier_semaphore()
    greet = [partner]
    greet += [plane(dx, dy) for dx in range(nxr) for dy in range(py) if dx + dy > 0]
    greet += [at(cc, xx, t % py, t // py) for t in ()]
    for t in range(1, ny):
        if t >= py:
            greet.append((gx, cold_peer(t, 1)))
    for device in greet:
        pl.semaphore_signal(barrier, inc=1, device_id=device, device_id_type=MESH)
    slots_copy.start()
    ids_copy.start()
    for copy in hot_copies:
        copy.start()

    slots_copy.wait()
    owners = slotv.shape[0]
    sub = lax.broadcasted_iota(jnp.int32, (owners, LANES), 0)
    lane = lax.broadcasted_iota(jnp.int32, (owners, LANES), 1)
    count = jnp.zeros((owners, LANES), jnp.int32)
    for o in range(owners):
        count = jnp.where(sub == o, counts_ref[o], count)
    for j in range(sstage.shape[1]):
        if j < cap_pieces:
            sstage[:, j, :] = jnp.where(lane + j * LANES < count, slotv[:, j * LANES : (j + 1) * LANES], -1)
        else:
            sstage[:, j, :] = jnp.full((owners, LANES), -1, jnp.int32)

    def cold_copies(t):
        peer = cold_peer(t, 1)
        return (
            pltpu.make_async_remote_copy(
                src_ref=cold_ref.at[peer], dst_ref=crecv.at[t],
                send_sem=csend.at[t], recv_sem=crsem.at[t],
                device_id=(gx, peer), device_id_type=MESH,
            ),
            pltpu.make_async_remote_copy(
                src_ref=sstage.at[peer], dst_ref=srecv.at[t],
                send_sem=ssend.at[t], recv_sem=srsem.at[t],
                device_id=(gx, peer), device_id_type=MESH,
            ),
        )

    def cold_start(ts):
        for t in ts:
            for copy in cold_copies(t):
                copy.start()

    def cold_add(ts, first=False):
        selectors, rows = [], []
        for t in ts:
            slots = sstage[gy] if t == 0 else srecv[t]
            low = jnp.bitwise_and(slots, own_low - 1)
            high = (slots >> bits(own_low)).T
            for j in range(cap_pieces):
                selectors.append(one_hot(jnp.broadcast_to(low[j : j + 1, :], (16, LANES)).astype(i16), own_low))
                code = jnp.broadcast_to(high[:, j : j + 1], (LANES, LANES)).astype(i16)
                rows.append(spread(code, crecv[t, j * LANES : (j + 1) * LANES, :], range(HIGH)))
        total = jnp.dot(
            jnp.concatenate(selectors, axis=1), jnp.concatenate(rows, axis=0), preferred_element_type=f32
        )
        for h in range(HIGH):
            part = total[:, h * LANES : (h + 1) * LANES]
            place = slice(h * own_low, (h + 1) * own_low)
            if first:
                cold_out[place, :] = part
            else:
                cold_out[place, :] += part

    def cold_take(ts):
        for t in ts:
            for copy in cold_copies(t):
                copy.wait()
        cold_add(ts)

    def split_ids(ids):
        row = ids & (piece - 1)
        rest = ids >> bits(piece)
        ch = rest & 1
        rest = rest >> 1
        z = ((rest & (nyr - 1)) - zz) & (nyr - 1)
        rest = rest >> bits(nyr)
        y = ((rest & (py - 1)) - yy) & (py - 1)
        rest = rest >> bits(py)
        x = ((rest & (nxr - 1)) - xx) & (nxr - 1)
        core = ((rest >> bits(nxr)) - cc) & 1
        top = jnp.where(ch == 0, x * py + y, y * nxr + x)
        place = (top * nyr + z) * piece + row
        return ch * half + (place & (half - 1)), core * 2 + (place >> bits(half))

    def hot_block(p, k):
        pieces = KBLOCK // LANES
        selectors, rows = [], []
        for q in range(pieces // 8):
            if p == 0:
                low, code = split_ids(idsv[k * pieces // 8 + q])
                columns = code.T
            for j in range(8):
                i = k * pieces + q * 8 + j
                here = slice(i * LANES, (i + 1) * LANES)
                if p == 0:
                    low_row = jnp.broadcast_to(low[j : j + 1, :], (16, LANES)).astype(i16)
                    column = jnp.broadcast_to(columns[:, j : j + 1], (LANES, LANES)).astype(i16)
                    lows[i] = low_row
                    codes[here, :] = column
                else:
                    low_row = lows[i]
                    column = codes[here, :]
                selectors.append(one_hot(low_row, chain))
                rows.append(spread(column, hotv[here, :], (1 - p, 3 - p)))
        total = jnp.dot(
            jnp.concatenate(selectors, axis=1), jnp.concatenate(rows, axis=0), preferred_element_type=f32
        )
        where = slice((1 - p) * half, (2 - p) * half)
        for c in range(2):
            part = total[c * half : (c + 1) * half, :LANES]
            if k == 0:
                tab[c, where, :] = part
            else:
                tab[c, where, :] += part
        if k == 0:
            give[p] = total[:, LANES:]
        else:
            give[p] += total[:, LANES:]

    used = [0]
    sent = []

    def send(src, dst, device):
        copy = pltpu.make_async_remote_copy(
            src_ref=src, dst_ref=dst, send_sem=hsend.at[used[0]], recv_sem=hrecv.at[used[0]],
            device_id=device, device_id_type=MESH,
        )
        used[0] += 1
        copy.start()
        sent.append(copy)
        return copy

    def arrival(ref, index):
        return pltpu.make_async_remote_copy(
            src_ref=ref, dst_ref=ref, send_sem=hsend.at[index], recv_sem=hrecv.at[index],
            device_id=partner, device_id_type=MESH,
        )

    stage1 = [(nxr, near_x, l1a), (py, near_y, l1b)]
    stage2 = [(py, near_y, l2a), (nxr, near_x, l2b)]
    stage3 = [(nyr, near_z, l3a), (nyr, near_z, l3b)]

    def stage1_sends(js):
        copies = {}
        for early in (True, False):
            for c in range(2):
                n, near, landing = stage1[c]
                size = chain // n
                keep = size // stage2[c][0]
                for j in js(n):
                    lo, hi = (keep, size) if early else (0, keep)
                    copies[early, c, j] = send(
                        tab.at[c, pl.ds(j * size + lo, hi - lo), :],
                        landing.at[j - 1, pl.ds(lo, hi - lo), :], near(j),
                    )
        return copies

    def add_take(p):
        where = slice((1 - p) * half, (2 - p) * half)
        for c in range(2):
            tab[c, where, :] += take[p, c * half : (c + 1) * half, :]

    pl.semaphore_wait(barrier, len(greet))
    cold_start(waves[0])
    own_copy.start()
    ids_copy.wait()
    for k in range(kblocks):
        hot_copies[k].wait()
        hot_block(0, k)
    core0 = send(give.at[0], take.at[0], partner)
    hot_block(1, 0)
    core0.wait_recv()
    add_take(0)
    first = stage1_sends(lambda n: range(n - 1, n // 2 - 1, -1))
    for k in range(1, kblocks):
        hot_block(1, k)
    core1 = send(give.at[1], take.at[1], partner)
    own_copy.wait()
    cold_add([0], first=True)
    core1.wait_recv()
    add_take(1)
    first.update(stage1_sends(lambda n: range(n // 2 - 1, 0, -1)))
    second = {}
    for early in (True, False):
        for c in range(2):
            n, _, landing = stage1[c]
            size = chain // n
            keep = size // stage2[c][0]
            lo, hi = (keep, size) if early else (0, keep)
            for j in range(1, n):
                first[early, c, j].wait_recv()
            for j in range(1, n):
                tab[c, lo:hi, :] += landing[j - 1, lo:hi, :]
            if early:
                n2, near, landing2 = stage2[c]
                for j in range(1, n2):
                    second[c, j] = send(tab.at[c, pl.ds(j * keep, keep), :], landing2.at[j - 1], near(j))
    third = {}
    for c in range(2):
        n, _, landing = stage2[c]
        size = chain // stage1[c][0] // n
        for j in range(1, n):
            second[c, j].wait_recv()
        for j in range(1, n):
            tab[c, :size, :] += landing[j - 1]
        n3, near, landing3 = stage3[c]
        for j in range(1, n3):
            third[c, j] = send(tab.at[c, pl.ds(j * piece, piece), :], landing3.at[j - 1], near(j))
    cold_start(waves[1])
    for group in waves[3]:
        cold_take(group)

    def block(c, x, y, z):
        index = ((c * nxr + x) * py + y) * nyr + z
        return pl.ds(pl.multiple_of(index * 2 * piece, 2 * piece), 2 * piece)

    base = (((cc * nxr + xx) * py + yy) * nyr + zz) * 2 * piece
    for c in range(2):
        n3, _, landing3 = stage3[c]
        for j in range(1, n3):
            third[c, j].wait_recv()
        total = tab[c, :piece, :]
        for j in range(1, n3):
            total = total + landing3[j - 1]
        hot_out[pl.ds(pl.multiple_of(base + c * piece, 8), piece), :] = total * factor

    def out(rows):
        return hot_out.at[rows, :]

    own = out(block(cc, xx, yy, zz))
    z_index = used[0]
    for j in range(1, nyr):
        send(own, own, near_z(j))
    plane_steps = [(dx, dy) for dx in range(nxr) for dy in range(py) if dx + dy > 0]
    plane_index, core_index = {}, {}

    def pass_on(j):
        rows = out(block(cc, xx, yy, lax.rem(zz + j, nyr)))
        for dx, dy in plane_steps:
            plane_index[dx, dy, j] = used[0]
            send(rows, rows, plane(dx, dy))
        core_index[0, 0, j] = used[0]
        send(rows, rows, partner)

    pass_on(0)
    cold_start(waves[2])
    order = sorted(range(1, nyr), key=lambda j: min(j, nyr - j))
    for j in order:
        rows = out(block(cc, xx, yy, lax.rem(zz + j, nyr)))
        arrival(rows, z_index + nyr - j - 1).wait_recv()
        pass_on(j)
    for group in waves[4]:
        cold_take(group)
    for j in [0] + order:
        for dx, dy in plane_steps:
            rows = out(block(cc, lax.rem(xx - dx + nxr, nxr), lax.rem(yy - dy + py, py), lax.rem(zz + j, nyr)))
            arrival(rows, plane_index[dx, dy, j]).wait_recv()
            core_index[dx, dy, j] = used[0]
            send(rows, rows, partner)
    for group in waves[5]:
        cold_take(group)
    for (dx, dy, j), index in core_index.items():
        rows = out(block(1 - cc, lax.rem(xx - dx + nxr, nxr), lax.rem(yy - dy + py, py), lax.rem(zz + j, nyr)))
        arrival(rows, index).wait_recv()
    for copy in sent:
        copy.wait_send()


def make_waves(ny, py):
    every = list(range(1, ny))
    if ny != 8:
        return [every[: ny // 2], [], every[ny // 2 :], [[t] for t in every[: ny // 2]], [], [[t] for t in every[ny // 2 :]]]
    return [[4, 2, 6], [], [5, 3, 7, 1], [[4, 2], [6]], [], [[5, 3], [7, 1]]]


def per_device(nx, ny, hot_ids, hot_grads, cold_grads, cold_slots, cold_counts):
    look, width = hot_grads.shape
    owners, capacity = cold_slots.shape[2], cold_slots.shape[3]
    px, py = 2, 2
    nxr, nyr = nx // px, ny // py
    factor = (HOT / (look * nx * ny)) ** 0.5
    chain = HOT // px // 2
    piece = chain // (nxr * ny)
    cap_pieces = capacity // LANES
    ids = hot_ids.reshape(-1, 8, LANES)
    n_sends = 2 + 4 * (nxr - 1) + 2 + 4 * (py - 1) + 3 * nyr + nxr * py * nyr * 2 + 8
    hbm = pl.BlockSpec(memory_space=pltpu.HBM)
    vmem = pl.BlockSpec(memory_space=pltpu.VMEM)
    smem = pl.BlockSpec(memory_space=pltpu.SMEM)
    dma = pltpu.SemaphoreType.DMA
    hot, cold = pl.pallas_call(
        functools.partial(kernel, nx, ny, factor, make_waves(ny, py)),
        out_shape=(
            jax.ShapeDtypeStruct((HOT, width), f32),
            jax.ShapeDtypeStruct((OWN_ROWS, width), f32),
        ),
        in_specs=[hbm, hbm, hbm, smem, hbm],
        out_specs=(vmem, vmem),
        scratch_shapes=[
            pltpu.VMEM((look, width), bf16),
            pltpu.VMEM(ids.shape, jnp.int32),
            pltpu.VMEM((look, LANES), i16),
            pltpu.VMEM((look // LANES, 16, LANES), i16),
            pltpu.VMEM((owners, capacity), jnp.int32),
            pltpu.VMEM((owners, -(-cap_pieces // 8) * 8, LANES), jnp.int32),
            pltpu.VMEM((owners, capacity, width), bf16),
            pltpu.VMEM((owners, -(-cap_pieces // 8) * 8, LANES), jnp.int32),
            pltpu.VMEM((2, chain, width), f32),
            pltpu.VMEM((8, width), f32),
            pltpu.VMEM((2, chain, width), f32),
            pltpu.VMEM((2, chain, width), f32),
            pltpu.VMEM((nxr - 1, chain // nxr, width), f32),
            pltpu.VMEM((py - 1, chain // py, width), f32),
            pltpu.VMEM((py - 1, chain // nxr // py, width), f32),
            pltpu.VMEM((nxr - 1, chain // nxr // py, width), f32),
            pltpu.VMEM((nyr - 1, piece, width), f32),
            pltpu.VMEM((nyr - 1, piece, width), f32),
            dma((3 + look // KBLOCK,)),
            dma((owners,)),
            dma((owners,)),
            dma((owners,)),
            dma((owners,)),
            dma((n_sends,)),
            dma((n_sends,)),
        ],
        compiler_params=pltpu.CompilerParams(
            collective_id=0, has_side_effects=True, vmem_limit_bytes=VMEM_KIB * 1024
        ),
    )(*(
        pltpu.with_memory_space_constraint(x, pltpu.HBM)
        for x in (ids, hot_grads, cold_slots.reshape(owners, capacity), cold_counts.reshape(owners), cold_grads.reshape(owners, capacity, width))
    ))
    return hot, cold.reshape(1, OWN_ROWS, width)


VMEM_KIB = 40000


def solution(mesh):
    body = functools.partial(per_device, mesh.shape["gx"], mesh.shape["gy"])
    return jax.shard_map(
        body,
        mesh=mesh,
        in_specs=(
            P(("gx", "gy")),
            P(("gx", "gy"), None),
            P("gx", "gy", None, None, None),
            P("gx", "gy", None, None),
            P("gx", "gy", None),
        ),
        out_specs=(P(), P("gx", "gy", None)),
        check_vma=False,
    )
```

```python
import functools

import jax
import jax.numpy as jnp
from jax import lax
from jax.experimental import pallas as pl
from jax.experimental.pallas import tpu as pltpu
from jax.sharding import PartitionSpec as P

HOT = 2048
OWN_ROWS = 2048
LANES = 128
HIGH = 4
KBLOCK = 4096
MESH = pl.DeviceIdType.MESH
bf16, f32, i16 = jnp.bfloat16, jnp.float32, jnp.int16


def bits(n):
    assert n & (n - 1) == 0
    return n.bit_length() - 1


def one_hot(row, size):
    places = lax.broadcasted_iota(jnp.int32, (size, LANES), 0).astype(i16)
    return jnp.where(places == jnp.concatenate([row] * (size // 16), axis=0), bf16(1), bf16(0))


def spread(codes, data, wanted):
    return jnp.concatenate(
        [jnp.where(codes == i16(w), data, jnp.zeros_like(data)) for w in wanted], axis=1
    )


def kernel(
    nx, ny, factor, sends, takes,
    ids_ref, hot_ref, slots_ref, counts_ref, cold_ref, hot_out, cold_out,
    hotv, idsv, codes, lows, slotv, sstage, crecv, srecv, tab, give, take,
    l1a, l1b, l2a, l2b, l3a, l3b, coded, scales, counts_smem, fence_sem,
    local_sem, csend, crsem, ssend, srsem, hsend, hrecv,
):
    gx, gy = lax.axis_index("gx"), lax.axis_index("gy")
    px, py = 2, 2
    nxr, nyr = nx // px, ny // py
    cc, xx = lax.rem(gx, px), gx // px
    yy, zz = lax.rem(gy, py), gy // py
    piece = HOT // (2 * nx * ny)
    chain = HOT // px // 2
    half = chain // 2
    kblocks = hotv.shape[0] // KBLOCK
    cap_pieces = crecv.shape[1] // LANES
    own_low = OWN_ROWS // HIGH

    def at(c, x, y, z):
        return (x * px + c, z * py + y)

    def near_x(j):
        return at(cc, lax.rem(xx + j, nxr), yy, zz)

    def near_y(j):
        return at(cc, xx, lax.rem(yy + j, py), zz)

    def near_z(j):
        return at(cc, xx, yy, lax.rem(zz + j, nyr))

    def plane(dx, dy):
        return at(cc, lax.rem(xx + dx, nxr), lax.rem(yy + dy, py), zz)

    partner = at(1 - cc, xx, yy, zz)

    def cold_peer(t, sign):
        da, db = t // py, t % py
        a = lax.rem(zz + sign * da + nyr, nyr)
        b = lax.rem(yy + sign * db + py, py)
        return a * py + b

    ids_copy = pltpu.make_async_copy(ids_ref, idsv, local_sem.at[0])
    slots_copy = pltpu.make_async_copy(slots_ref, slotv, local_sem.at[1])
    counts_copy = pltpu.make_async_copy(counts_ref, counts_smem, local_sem.at[3])
    own_copy = pltpu.make_async_copy(cold_ref.at[gy], crecv.at[0], local_sem.at[2])
    hot_copies = [
        pltpu.make_async_copy(
            hot_ref.at[pl.ds(k * KBLOCK, KBLOCK), :], hotv.at[pl.ds(k * KBLOCK, KBLOCK), :], local_sem.at[4 + k]
        )
        for k in range(kblocks)
    ]
    barrier = pltpu.get_barrier_semaphore()
    greet = [partner]
    greet += [plane(dx, dy) for dx in range(nxr) for dy in range(py) if dx + dy > 0]
    for t in range(1, ny):
        if t >= py:
            greet.append((gx, cold_peer(t, 1)))
    for device in greet:
        pl.semaphore_signal(barrier, inc=1, device_id=device, device_id_type=MESH)
    counts_copy.start()
    slots_copy.start()
    ids_copy.start()
    for copy in hot_copies:
        copy.start()
    pl.semaphore_wait(barrier, len(greet))

    def cold_copy(t, part):
        peer = cold_peer(t, 1)
        source, landing, send_sem, recv_sem = (
            (cold_ref, crecv, csend, crsem) if part == 0 else (sstage, srecv, ssend, srsem)
        )
        return pltpu.make_async_remote_copy(
            src_ref=source.at[peer], dst_ref=landing.at[t],
            send_sem=send_sem.at[t], recv_sem=recv_sem.at[t],
            device_id=(gx, peer), device_id_type=MESH,
        )

    def cold_start(ts, parts=(1, 0)):
        for part in parts:
            for t in ts:
                cold_copy(t, part).start()

    def fence():
        pl.semaphore_signal(fence_sem, 1)
        pl.semaphore_wait(fence_sem, 1)

    def cold_add(ts, first=False):
        selectors, rows = [], []
        for t in ts:
            slots = sstage[gy] if t == 0 else srecv[t]
            low = jnp.bitwise_and(slots, own_low - 1)
            high = (slots >> bits(own_low)).T
            for j in range(cap_pieces):
                selectors.append(one_hot(jnp.broadcast_to(low[j : j + 1, :], (16, LANES)).astype(i16), own_low))
                code = jnp.broadcast_to(high[:, j : j + 1], (LANES, LANES)).astype(i16)
                rows.append(spread(code, crecv[t, j * LANES : (j + 1) * LANES, :], range(HIGH)))
        total = jnp.dot(
            jnp.concatenate(selectors, axis=1), jnp.concatenate(rows, axis=0), preferred_element_type=f32
        )
        for h in range(HIGH):
            part = total[:, h * LANES : (h + 1) * LANES]
            place = slice(h * own_low, (h + 1) * own_low)
            if first:
                cold_out[place, :] = part
            else:
                cold_out[place, :] += part

    def cold_take(ts):
        for t in ts:
            for part in range(2):
                cold_copy(t, part).wait()
        cold_add(ts)

    def split_ids(ids):
        row = ids & (piece - 1)
        rest = ids >> bits(piece)
        ch = rest & 1
        rest = rest >> 1
        z = ((rest & (nyr - 1)) - zz) & (nyr - 1)
        rest = rest >> bits(nyr)
        y = ((rest & (py - 1)) - yy) & (py - 1)
        rest = rest >> bits(py)
        x = ((rest & (nxr - 1)) - xx) & (nxr - 1)
        core = ((rest >> bits(nxr)) - cc) & 1
        top = jnp.where(ch == 0, x * py + y, y * nxr + x)
        place = (top * nyr + z) * piece + row
        return ch * half + (place & (half - 1)), core * 2 + (place >> bits(half))

    def hot_block(p, k):
        pieces = KBLOCK // LANES
        selectors, rows = [], []
        for q in range(pieces // 8):
            if p == 0:
                low, code = split_ids(idsv[k * pieces // 8 + q])
                columns = code.T
            for j in range(8):
                i = k * pieces + q * 8 + j
                here = slice(i * LANES, (i + 1) * LANES)
                if p == 0:
                    low_row = jnp.broadcast_to(low[j : j + 1, :], (16, LANES)).astype(i16)
                    column = jnp.broadcast_to(columns[:, j : j + 1], (LANES, LANES)).astype(i16)
                    lows[i] = low_row
                    codes[here, :] = column
                else:
                    low_row = lows[i]
                    column = codes[here, :]
                selectors.append(one_hot(low_row, chain))
                rows.append(spread(column, hotv[here, :], (1 - p, 3 - p)))
        total = jnp.dot(
            jnp.concatenate(selectors, axis=1), jnp.concatenate(rows, axis=0), preferred_element_type=f32
        )
        where = slice((1 - p) * half, (2 - p) * half)
        for c in range(2):
            part = total[c * half : (c + 1) * half, :LANES]
            if k == 0:
                tab[c, where, :] = part
            else:
                tab[c, where, :] += part
        if k == 0:
            give[p] = total[:, LANES:]
        else:
            give[p] += total[:, LANES:]

    used = [0]
    sent = []

    def send(src, dst, device):
        copy = pltpu.make_async_remote_copy(
            src_ref=src, dst_ref=dst, send_sem=hsend.at[used[0]], recv_sem=hrecv.at[used[0]],
            device_id=device, device_id_type=MESH,
        )
        used[0] += 1
        copy.start()
        sent.append(copy)
        return copy

    def arrival(ref, index):
        return pltpu.make_async_remote_copy(
            src_ref=ref, dst_ref=ref, send_sem=hsend.at[index], recv_sem=hrecv.at[index],
            device_id=partner, device_id_type=MESH,
        )

    stage1 = [(nxr, near_x, l1a), (py, near_y, l1b)]
    stage2 = [(py, near_y, l2a), (nxr, near_x, l2b)]
    stage3 = [(nyr, near_z, l3a), (nyr, near_z, l3b)]

    def stage1_sends(js):
        copies = {}
        for early in (True, False):
            for c in range(2):
                n, near, landing = stage1[c]
                size = chain // n
                keep = size // stage2[c][0]
                for j in js(n):
                    lo, hi = (keep, size) if early else (0, keep)
                    copies[early, c, j] = send(
                        tab.at[c, pl.ds(j * size + lo, hi - lo), :],
                        landing.at[j - 1, pl.ds(lo, hi - lo), :], near(j),
                    )
        return copies

    def add_take(p):
        where = slice((1 - p) * half, (2 - p) * half)
        for c in range(2):
            tab[c, where, :] += take[p, c * half : (c + 1) * half, :]

    cold_start(sends[0], (0,))
    own_copy.start()
    counts_copy.wait()
    slots_copy.wait()
    owners = slotv.shape[0]
    sub = lax.broadcasted_iota(jnp.int32, (owners, LANES), 0)
    lane = lax.broadcasted_iota(jnp.int32, (owners, LANES), 1)
    count = jnp.zeros((owners, LANES), jnp.int32)
    for o in range(owners):
        count = jnp.where(sub == o, counts_smem[o], count)
    for j in range(sstage.shape[1]):
        if j < cap_pieces:
            sstage[:, j, :] = jnp.where(lane + j * LANES < count, slotv[:, j * LANES : (j + 1) * LANES], -1)
        else:
            sstage[:, j, :] = jnp.full((owners, LANES), -1, jnp.int32)

    cold_start(sends[0], (1,))
    ids_copy.wait()
    for k in range(kblocks):
        hot_copies[k].wait()
        hot_block(0, k)
    core0 = send(give.at[0], take.at[0], partner)
    cold_start(sends[1])
    fence()
    hot_block(1, 0)
    core0.wait_recv()
    add_take(0)
    first = stage1_sends(lambda n: range(n - 1, n // 2 - 1, -1))
    cold_start(sends[2])
    fence()
    for k in range(1, kblocks):
        hot_block(1, k)
    core1 = send(give.at[1], take.at[1], partner)
    cold_start(sends[3])
    fence()
    own_copy.wait()
    cold_add([0], first=True)
    core1.wait_recv()
    add_take(1)
    first.update(stage1_sends(lambda n: range(n // 2 - 1, 0, -1)))
    second = {}
    for early in (True, False):
        for c in range(2):
            n, _, landing = stage1[c]
            size = chain // n
            keep = size // stage2[c][0]
            lo, hi = (keep, size) if early else (0, keep)
            for j in range(1, n):
                first[early, c, j].wait_recv()
            for j in range(1, n):
                tab[c, lo:hi, :] += landing[j - 1, lo:hi, :]
            if early:
                n2, near, landing2 = stage2[c]
                for j in range(1, n2):
                    second[c, j] = send(tab.at[c, pl.ds(j * keep, keep), :], landing2.at[j - 1], near(j))
    cold_start(sends[4])
    third = {}
    for c in range(2):
        n, _, landing = stage2[c]
        size = chain // stage1[c][0] // n
        for j in range(1, n):
            second[c, j].wait_recv()
        for j in range(1, n):
            tab[c, :size, :] += landing[j - 1]
        n3, near, landing3 = stage3[c]
        for j in range(1, n3):
            third[c, j] = send(tab.at[c, pl.ds(j * piece, piece), :], landing3.at[j - 1], near(j))
    cold_start(sends[5])
    for group in takes[0]:
        cold_take(group)

    def block(c, x, y, z):
        return ((c * nxr + x) * py + y) * nyr + z

    rows = 2 * piece
    groups = rows // 8
    eye = [
        lax.broadcasted_iota(jnp.int32, (8, LANES), 1)
        == lax.broadcasted_iota(jnp.int32, (8, LANES), 0) + g * 8
        for g in range(groups)
    ]
    totals = []
    for c in range(2):
        n3, _, landing3 = stage3[c]
        for j in range(1, n3):
            third[c, j].wait_recv()
        total = tab[c, :piece, :]
        for j in range(1, n3):
            total = total + landing3[j - 1]
        totals.append(total)
    total = jnp.concatenate(totals, axis=0) * factor
    largest = jnp.max(jnp.abs(total), axis=1, keepdims=True)
    unit = jnp.where(largest > 0, 32767.0 / largest, 0.0)
    steps = jnp.round(jnp.clip(total * unit, -32767.0, 32767.0)).astype(jnp.int32).astype(i16)
    mine = block(cc, xx, yy, zz)
    coded[mine] = steps
    size = jnp.broadcast_to(largest * (1.0 / 32767.0), (rows, LANES))
    row = jnp.zeros((8, LANES), f32)
    for g in range(groups):
        row = row + jnp.where(eye[g], size[g * 8 : (g + 1) * 8, :], 0.0)
    scales[mine] = jnp.sum(row, axis=0, keepdims=True)

    def decode(index):
        row = jnp.broadcast_to(scales[index], (8, LANES))
        value = coded[index].astype(jnp.int32).astype(f32)
        for g in range(groups):
            size = jnp.sum(jnp.where(eye[g], row, 0.0), axis=1, keepdims=True)
            hot_out[pl.ds(pl.multiple_of(index * rows + g * 8, 8), 8), :] = value[g * 8 : (g + 1) * 8, :] * size

    def share(place, device):
        index = used[0]
        for ref in (scales, coded):
            send(ref.at[place], ref.at[place], device)
        return index

    def arrived(place, index):
        for n, ref in enumerate((scales, coded)):
            arrival(ref.at[place], index + n).wait_recv()

    z_index = {j: share(mine, near_z(j)) for j in range(1, nyr)}
    plane_steps = [(dx, dy) for dx in range(nxr) for dy in range(py) if dx + dy > 0]
    plane_index, core_index = {}, {}

    def column(c, x, y):
        return pl.ds(block(c, x, y, 0), nyr)

    def from_plane(dx, dy):
        return lax.rem(xx - dx + nxr, nxr), lax.rem(yy - dy + py, py)

    def pass_on(j):
        for dx, dy in plane_steps:
            plane_index[dx, dy, j] = share(block(cc, xx, yy, lax.rem(zz + j, nyr)), plane(dx, dy))

    cold_start(sends[6])
    pass_on(0)
    cold_start(sends[7])
    order = sorted(range(1, nyr), key=lambda j: min(j, nyr - j))
    for j in order:
        arrived(block(cc, xx, yy, lax.rem(zz + j, nyr)), z_index[nyr - j])
        pass_on(j)
    core_index[0, 0] = share(column(cc, xx, yy), partner)
    cold_start(sends[8])
    for group in takes[1]:
        cold_take(group)
    for j in [0] + order:
        decode(block(cc, xx, yy, lax.rem(zz + j, nyr)))
    for dx, dy in plane_steps:
        x, y = from_plane(dx, dy)
        for j in [0] + order:
            arrived(block(cc, x, y, lax.rem(zz + j, nyr)), plane_index[dx, dy, j])
        core_index[dx, dy] = share(column(cc, x, y), partner)
        for z in range(nyr):
            decode(block(cc, x, y, z))
    for group in takes[2]:
        cold_take(group)
    for (dx, dy), index in core_index.items():
        x, y = from_plane(dx, dy)
        arrived(column(1 - cc, x, y), index)
        for z in range(nyr):
            decode(block(1 - cc, x, y, z))
    for copy in sent:
        copy.wait_send()


def make_waves(ny):
    if ny == 8:
        return SENDS, TAKES
    every = list(range(1, ny))
    early, late = every[: ny // 2], every[ny // 2 :]
    return [early, [], [], [], [], [], [], late, []], [[[t] for t in early], [], [[t] for t in late]]


SENDS = [[5, 3, 1], [], [], [4], [], [], [], [2, 6, 7], []]
TAKES = [[[5, 3]], [], [[4, 1], [7, 2], [6]]]


def per_device(nx, ny, hot_ids, hot_grads, cold_grads, cold_slots, cold_counts):
    look, width = hot_grads.shape
    owners, capacity = cold_slots.shape[2], cold_slots.shape[3]
    px, py = 2, 2
    nxr, nyr = nx // px, ny // py
    factor = (HOT / (look * nx * ny)) ** 0.5
    chain = HOT // px // 2
    piece = chain // (nxr * ny)
    cap_pieces = capacity // LANES
    ids = hot_ids.reshape(-1, 8, LANES)
    n_sends = 2 + 3 * (nxr - 1) + 3 * (py - 1) + 4 * (nyr - 1) + 2 * (nxr * py - 1) * nyr + 2 * nxr * py
    hbm = pl.BlockSpec(memory_space=pltpu.HBM)
    vmem = pl.BlockSpec(memory_space=pltpu.VMEM)
    dma = pltpu.SemaphoreType.DMA
    hot, cold = pl.pallas_call(
        functools.partial(kernel, nx, ny, factor, *make_waves(ny)),
        out_shape=(
            jax.ShapeDtypeStruct((HOT, width), f32),
            jax.ShapeDtypeStruct((OWN_ROWS, width), f32),
        ),
        in_specs=[hbm, hbm, hbm, hbm, hbm],
        out_specs=(vmem, vmem),
        scratch_shapes=[
            pltpu.VMEM((look, width), bf16),
            pltpu.VMEM(ids.shape, jnp.int32),
            pltpu.VMEM((look, LANES), i16),
            pltpu.VMEM((look // LANES, 16, LANES), i16),
            pltpu.VMEM((owners, capacity), jnp.int32),
            pltpu.VMEM((owners, -(-cap_pieces // 8) * 8, LANES), jnp.int32),
            pltpu.VMEM((owners, capacity, width), bf16),
            pltpu.VMEM((owners, -(-cap_pieces // 8) * 8, LANES), jnp.int32),
            pltpu.VMEM((2, chain, width), f32),
            pltpu.VMEM((2, chain, width), f32),
            pltpu.VMEM((2, chain, width), f32),
            pltpu.VMEM((nxr - 1, chain // nxr, width), f32),
            pltpu.VMEM((py - 1, chain // py, width), f32),
            pltpu.VMEM((py - 1, chain // nxr // py, width), f32),
            pltpu.VMEM((nxr - 1, chain // nxr // py, width), f32),
            pltpu.VMEM((nyr - 1, piece, width), f32),
            pltpu.VMEM((nyr - 1, piece, width), f32),
            pltpu.VMEM((nx * ny, 2 * piece, width), i16),
            pltpu.VMEM((nx * ny, 1, LANES), f32),
            pltpu.SMEM((owners,), jnp.int32),
            pltpu.SemaphoreType.REGULAR,
            dma((4 + look // KBLOCK,)),
            dma((owners,)),
            dma((owners,)),
            dma((owners,)),
            dma((owners,)),
            dma((n_sends,)),
            dma((n_sends,)),
        ],
        compiler_params=pltpu.CompilerParams(
            collective_id=0, has_side_effects=True, vmem_limit_bytes=VMEM_KIB * 1024
        ),
    )(*(
        pltpu.with_memory_space_constraint(x, pltpu.HBM)
        for x in (ids, hot_grads, cold_slots.reshape(owners, capacity), cold_counts.reshape(owners), cold_grads.reshape(owners, capacity, width))
    ))
    return hot, cold.reshape(1, OWN_ROWS, width)


VMEM_KIB = 40000


def solution(mesh):
    body = functools.partial(per_device, mesh.shape["gx"], mesh.shape["gy"])
    return jax.shard_map(
        body,
        mesh=mesh,
        in_specs=(
            P(("gx", "gy")),
            P(("gx", "gy"), None),
            P("gx", "gy", None, None, None),
            P("gx", "gy", None, None),
            P("gx", "gy", None),
        ),
        out_specs=(P(), P("gx", "gy", None)),
        check_vma=False,
    )
```

```python
import functools

import jax
import jax.numpy as jnp
from jax import lax
from jax.experimental import pallas as pl
from jax.experimental.pallas import tpu as pltpu
from jax.sharding import PartitionSpec as P

HOT = 2048
OWN_ROWS = 2048
LANES = 128
HIGH = 4
KBLOCK = 4096
MESH = pl.DeviceIdType.MESH
bf16, f32, i16 = jnp.bfloat16, jnp.float32, jnp.int16


def bits(n):
    assert n & (n - 1) == 0
    return n.bit_length() - 1


def one_hot(row, size):
    places = lax.broadcasted_iota(jnp.int32, (size, LANES), 0).astype(i16)
    return jnp.where(places == jnp.concatenate([row] * (size // 16), axis=0), bf16(1), bf16(0))


def spread(codes, data, wanted):
    return jnp.concatenate(
        [jnp.where(codes == i16(w), data, jnp.zeros_like(data)) for w in wanted], axis=1
    )


def kernel(
    nx, ny, factor, sends, takes,
    ids_ref, hot_ref, slots_ref, counts_ref, cold_ref, hot_out, cold_out,
    hotv, idsv, codes, lows, slotv, sstage, crecv, srecv, tab, give, take,
    l1a, l1b, l2a, l2b, l3a, l3b, coded, scales, counts_smem, fence_sem,
    local_sem, csend, crsem, hsend, hrecv,
):
    gx, gy = lax.axis_index("gx"), lax.axis_index("gy")
    px, py = 2, 2
    nxr, nyr = nx // px, ny // py
    cc, xx = lax.rem(gx, px), gx // px
    yy, zz = lax.rem(gy, py), gy // py
    piece = HOT // (2 * nx * ny)
    chain = HOT // px // 2
    half = chain // 2
    kblocks = hotv.shape[0] // KBLOCK
    cap_pieces = crecv.shape[1] // LANES
    own_low = OWN_ROWS // HIGH

    def at(c, x, y, z):
        return (x * px + c, z * py + y)

    def near_x(j):
        return at(cc, lax.rem(xx + j, nxr), yy, zz)

    def near_y(j):
        return at(cc, xx, lax.rem(yy + j, py), zz)

    def near_z(j):
        return at(cc, xx, yy, lax.rem(zz + j, nyr))

    def plane(dx, dy):
        return at(cc, lax.rem(xx + dx, nxr), lax.rem(yy + dy, py), zz)

    partner = at(1 - cc, xx, yy, zz)

    def cold_peer(t, sign):
        da, db = t // py, t % py
        a = lax.rem(zz + sign * da + nyr, nyr)
        b = lax.rem(yy + sign * db + py, py)
        return a * py + b

    ids_copy = pltpu.make_async_copy(ids_ref, idsv, local_sem.at[0])
    slots_copy = pltpu.make_async_copy(slots_ref, slotv, local_sem.at[1])
    counts_copy = pltpu.make_async_copy(counts_ref, counts_smem, local_sem.at[3])
    own_copy = pltpu.make_async_copy(cold_ref.at[gy], crecv.at[0], local_sem.at[2])
    hot_copies = [
        pltpu.make_async_copy(
            hot_ref.at[pl.ds(k * KBLOCK, KBLOCK), :], hotv.at[pl.ds(k * KBLOCK, KBLOCK), :], local_sem.at[4 + k]
        )
        for k in range(kblocks)
    ]
    barrier = pltpu.get_barrier_semaphore()
    greet = [partner]
    greet += [plane(dx, dy) for dx in range(nxr) for dy in range(py) if dx + dy > 0]
    for t in range(1, ny):
        if t >= py:
            greet.append((gx, cold_peer(t, 1)))
    for device in greet:
        pl.semaphore_signal(barrier, inc=1, device_id=device, device_id_type=MESH)
    counts_copy.start()
    slots_copy.start()
    ids_copy.start()
    for copy in hot_copies:
        copy.start()
    pl.semaphore_wait(barrier, len(greet))

    halves = crecv.shape[1] // 2

    def cold_copy(t, part):
        peer = cold_peer(t, 1)
        if part < 2:
            rows = pl.ds(part * halves, halves)
            source, landing = cold_ref.at[peer, rows, :], crecv.at[t, rows, :]
        else:
            source, landing = sstage.at[peer], srecv.at[t]
        return pltpu.make_async_remote_copy(
            src_ref=source, dst_ref=landing,
            send_sem=csend.at[3 * t + part], recv_sem=crsem.at[3 * t + part],
            device_id=(gx, peer), device_id_type=MESH,
        )

    def cold_start(items):
        for item in items:
            if item % 2 == 0 and item not in sends[0]:
                cold_copy(item // 2, 2).start()
        for item in items:
            cold_copy(item // 2, item % 2).start()

    def fence():
        pl.semaphore_signal(fence_sem, 1)
        pl.semaphore_wait(fence_sem, 1)

    def cold_add(ts, first=False):
        selectors, rows = [], []
        for t in ts:
            slots = sstage[gy] if t == 0 else srecv[t]
            low = jnp.bitwise_and(slots, own_low - 1)
            high = (slots >> bits(own_low)).T
            for j in range(cap_pieces):
                selectors.append(one_hot(jnp.broadcast_to(low[j : j + 1, :], (16, LANES)).astype(i16), own_low))
                code = jnp.broadcast_to(high[:, j : j + 1], (LANES, LANES)).astype(i16)
                rows.append(spread(code, crecv[t, j * LANES : (j + 1) * LANES, :], range(HIGH)))
        total = jnp.dot(
            jnp.concatenate(selectors, axis=1), jnp.concatenate(rows, axis=0), preferred_element_type=f32
        )
        for h in range(HIGH):
            part = total[:, h * LANES : (h + 1) * LANES]
            place = slice(h * own_low, (h + 1) * own_low)
            if first:
                cold_out[place, :] = part
            else:
                cold_out[place, :] += part

    def cold_take(ts):
        for t in ts:
            for part in range(3):
                cold_copy(t, part).wait()
        cold_add(ts)

    def split_ids(ids):
        row = ids & (piece - 1)
        rest = ids >> bits(piece)
        ch = rest & 1
        rest = rest >> 1
        z = ((rest & (nyr - 1)) - zz) & (nyr - 1)
        rest = rest >> bits(nyr)
        y = ((rest & (py - 1)) - yy) & (py - 1)
        rest = rest >> bits(py)
        x = ((rest & (nxr - 1)) - xx) & (nxr - 1)
        core = ((rest >> bits(nxr)) - cc) & 1
        top = jnp.where(ch == 0, x * py + y, y * nxr + x)
        place = (top * nyr + z) * piece + row
        return ch * half + (place & (half - 1)), core * 2 + (place >> bits(half))

    def hot_block(p, k):
        pieces = KBLOCK // LANES
        selectors, rows = [], []
        for q in range(pieces // 8):
            if p == 0:
                low, code = split_ids(idsv[k * pieces // 8 + q])
                columns = code.T
            for j in range(8):
                i = k * pieces + q * 8 + j
                here = slice(i * LANES, (i + 1) * LANES)
                if p == 0:
                    low_row = jnp.broadcast_to(low[j : j + 1, :], (16, LANES)).astype(i16)
                    column = jnp.broadcast_to(columns[:, j : j + 1], (LANES, LANES)).astype(i16)
                    lows[i] = low_row
                    codes[here, :] = column
                else:
                    low_row = lows[i]
                    column = codes[here, :]
                selectors.append(one_hot(low_row, chain))
                rows.append(spread(column, hotv[here, :], (1 - p, 3 - p)))
        total = jnp.dot(
            jnp.concatenate(selectors, axis=1), jnp.concatenate(rows, axis=0), preferred_element_type=f32
        )
        where = slice((1 - p) * half, (2 - p) * half)
        for c in range(2):
            part = total[c * half : (c + 1) * half, :LANES]
            if k == 0:
                tab[c, where, :] = part
            else:
                tab[c, where, :] += part
        if k == 0:
            give[p] = total[:, LANES:]
        else:
            give[p] += total[:, LANES:]

    used = [0]
    sent = []

    def send(src, dst, device):
        copy = pltpu.make_async_remote_copy(
            src_ref=src, dst_ref=dst, send_sem=hsend.at[used[0]], recv_sem=hrecv.at[used[0]],
            device_id=device, device_id_type=MESH,
        )
        used[0] += 1
        copy.start()
        sent.append(copy)
        return copy

    def arrival(ref, index):
        return pltpu.make_async_remote_copy(
            src_ref=ref, dst_ref=ref, send_sem=hsend.at[index], recv_sem=hrecv.at[index],
            device_id=partner, device_id_type=MESH,
        )

    stage1 = [(nxr, near_x, l1a), (py, near_y, l1b)]
    stage2 = [(py, near_y, l2a), (nxr, near_x, l2b)]
    stage3 = [(nyr, near_z, l3a), (nyr, near_z, l3b)]

    def stage1_sends(js):
        copies = {}
        for early in (True, False):
            for c in range(2):
                n, near, landing = stage1[c]
                size = chain // n
                keep = size // stage2[c][0]
                for j in js(n):
                    lo, hi = (keep, size) if early else (0, keep)
                    copies[early, c, j] = send(
                        tab.at[c, pl.ds(j * size + lo, hi - lo), :],
                        landing.at[j - 1, pl.ds(lo, hi - lo), :], near(j),
                    )
        return copies

    def add_take(p):
        where = slice((1 - p) * half, (2 - p) * half)
        for c in range(2):
            tab[c, where, :] += take[p, c * half : (c + 1) * half, :]

    for item in sends[0]:
        cold_copy(item // 2, item % 2).start()
    own_copy.start()
    counts_copy.wait()
    slots_copy.wait()
    owners = slotv.shape[0]
    sub = lax.broadcasted_iota(jnp.int32, (owners, LANES), 0)
    lane = lax.broadcasted_iota(jnp.int32, (owners, LANES), 1)
    count = jnp.zeros((owners, LANES), jnp.int32)
    for o in range(owners):
        count = jnp.where(sub == o, counts_smem[o], count)
    for j in range(sstage.shape[1]):
        if j < cap_pieces:
            sstage[:, j, :] = jnp.where(lane + j * LANES < count, slotv[:, j * LANES : (j + 1) * LANES], -1)
        else:
            sstage[:, j, :] = jnp.full((owners, LANES), -1, jnp.int32)

    for item in sends[0]:
        if item % 2 == 0:
            cold_copy(item // 2, 2).start()
    ids_copy.wait()
    for k in range(kblocks):
        hot_copies[k].wait()
        hot_block(0, k)
    core0 = send(give.at[0], take.at[0], partner)
    cold_start(sends[1])
    fence()
    hot_block(1, 0)
    core0.wait_recv()
    add_take(0)
    first = stage1_sends(lambda n: range(n - 1, n // 2 - 1, -1))
    cold_start(sends[2])
    fence()
    for k in range(1, kblocks):
        hot_block(1, k)
    core1 = send(give.at[1], take.at[1], partner)
    cold_start(sends[3])
    fence()
    own_copy.wait()
    cold_add([0], first=True)
    core1.wait_recv()
    add_take(1)
    first.update(stage1_sends(lambda n: range(n // 2 - 1, 0, -1)))
    second = {}
    for early in (True, False):
        for c in range(2):
            n, _, landing = stage1[c]
            size = chain // n
            keep = size // stage2[c][0]
            lo, hi = (keep, size) if early else (0, keep)
            for j in range(1, n):
                first[early, c, j].wait_recv()
            for j in range(1, n):
                tab[c, lo:hi, :] += landing[j - 1, lo:hi, :]
            if early:
                n2, near, landing2 = stage2[c]
                for j in range(1, n2):
                    second[c, j] = send(tab.at[c, pl.ds(j * keep, keep), :], landing2.at[j - 1], near(j))
    cold_start(sends[4])
    third = {}
    for c in range(2):
        n, _, landing = stage2[c]
        size = chain // stage1[c][0] // n
        for j in range(1, n):
            second[c, j].wait_recv()
        for j in range(1, n):
            tab[c, :size, :] += landing[j - 1]
        n3, near, landing3 = stage3[c]
        for j in range(1, n3):
            third[c, j] = send(tab.at[c, pl.ds(j * piece, piece), :], landing3.at[j - 1], near(j))
    cold_start(sends[5])
    for group in takes[0]:
        cold_take(group)

    def block(c, x, y, z):
        return ((c * nxr + x) * py + y) * nyr + z

    rows = 2 * piece
    groups = rows // 8
    eye = [
        lax.broadcasted_iota(jnp.int32, (8, LANES), 1)
        == lax.broadcasted_iota(jnp.int32, (8, LANES), 0) + g * 8
        for g in range(groups)
    ]
    totals = []
    for c in range(2):
        n3, _, landing3 = stage3[c]
        for j in range(1, n3):
            third[c, j].wait_recv()
        total = tab[c, :piece, :]
        for j in range(1, n3):
            total = total + landing3[j - 1]
        totals.append(total)
    total = jnp.concatenate(totals, axis=0) * factor
    largest = jnp.max(jnp.abs(total), axis=1, keepdims=True)
    unit = jnp.where(largest > 0, 32767.0 / largest, 0.0)
    steps = jnp.round(jnp.clip(total * unit, -32767.0, 32767.0)).astype(jnp.int32).astype(i16)
    mine = block(cc, xx, yy, zz)
    coded[mine] = steps
    size = jnp.broadcast_to(largest * (1.0 / 32767.0), (rows, LANES))
    row = jnp.zeros((8, LANES), f32)
    for g in range(groups):
        row = row + jnp.where(eye[g], size[g * 8 : (g + 1) * 8, :], 0.0)
    scales[mine] = jnp.sum(row, axis=0, keepdims=True)

    def decode(index):
        row = jnp.broadcast_to(scales[index], (8, LANES))
        value = coded[index].astype(jnp.int32).astype(f32)
        for g in range(groups):
            size = jnp.sum(jnp.where(eye[g], row, 0.0), axis=1, keepdims=True)
            hot_out[pl.ds(pl.multiple_of(index * rows + g * 8, 8), 8), :] = value[g * 8 : (g + 1) * 8, :] * size

    def share(place, device):
        index = used[0]
        for ref in (scales, coded):
            send(ref.at[place], ref.at[place], device)
        return index

    def arrived(place, index):
        for n, ref in enumerate((scales, coded)):
            arrival(ref.at[place], index + n).wait_recv()

    z_index = {j: share(mine, near_z(j)) for j in range(1, nyr)}
    plane_steps = [(dx, dy) for dx in range(nxr) for dy in range(py) if dx + dy > 0]
    plane_index, core_index = {}, {}

    def column(c, x, y):
        return pl.ds(block(c, x, y, 0), nyr)

    def from_plane(dx, dy):
        return lax.rem(xx - dx + nxr, nxr), lax.rem(yy - dy + py, py)

    def pass_on(j):
        for dx, dy in plane_steps:
            plane_index[dx, dy, j] = share(block(cc, xx, yy, lax.rem(zz + j, nyr)), plane(dx, dy))

    cold_start(sends[6])
    pass_on(0)
    cold_start(sends[7])
    order = sorted(range(1, nyr), key=lambda j: min(j, nyr - j))
    for j in order:
        arrived(block(cc, xx, yy, lax.rem(zz + j, nyr)), z_index[nyr - j])
        pass_on(j)
    core_index[0, 0] = share(column(cc, xx, yy), partner)
    cold_start(sends[8])
    for group in takes[1]:
        cold_take(group)
    for j in [0] + order:
        decode(block(cc, xx, yy, lax.rem(zz + j, nyr)))
    for dx, dy in plane_steps:
        x, y = from_plane(dx, dy)
        for j in [0] + order:
            arrived(block(cc, x, y, lax.rem(zz + j, nyr)), plane_index[dx, dy, j])
        core_index[dx, dy] = share(column(cc, x, y), partner)
        for z in range(nyr):
            decode(block(cc, x, y, z))
    for group in takes[2]:
        cold_take(group)
    for (dx, dy), index in core_index.items():
        x, y = from_plane(dx, dy)
        arrived(column(1 - cc, x, y), index)
        for z in range(nyr):
            decode(block(1 - cc, x, y, z))
    for copy in sent:
        copy.wait_send()


def store(hot_ref, cold_ref, hot_out, cold_out, sem):
    copies = [
        pltpu.make_async_copy(hot_ref, hot_out, sem.at[0]),
        pltpu.make_async_copy(cold_ref, cold_out, sem.at[1]),
    ]
    for copy in copies:
        copy.start()
    for copy in copies:
        copy.wait()


def make_waves(ny):
    if ny == 8:
        return SENDS, TAKES
    every = list(range(1, ny))
    early, late = every[: ny // 2], every[ny // 2 :]
    both = lambda ts: [2 * t + h for t in ts for h in range(2)]
    return [both(early), [], [], [], [], [], [], both(late), []], [[[t] for t in early], [], [[t] for t in late]]


SENDS = [[2, 3, 6, 7, 10, 11], [], [], [8, 9], [], [], [], [4, 5, 12, 13, 14, 15], []]
TAKES = [[[1, 3]], [], [[5, 4], [2, 6], [7]]]


def per_device(nx, ny, hot_ids, hot_grads, cold_grads, cold_slots, cold_counts):
    look, width = hot_grads.shape
    owners, capacity = cold_slots.shape[2], cold_slots.shape[3]
    px, py = 2, 2
    nxr, nyr = nx // px, ny // py
    factor = (HOT / (look * nx * ny)) ** 0.5
    chain = HOT // px // 2
    piece = chain // (nxr * ny)
    cap_pieces = capacity // LANES
    ids = hot_ids.reshape(-1, 8, LANES)
    n_sends = 2 + 3 * (nxr - 1) + 3 * (py - 1) + 4 * (nyr - 1) + 2 * (nxr * py - 1) * nyr + 2 * nxr * py
    hbm = pl.BlockSpec(memory_space=pltpu.HBM)
    vmem = pl.BlockSpec(memory_space=pltpu.VMEM)
    dma = pltpu.SemaphoreType.DMA
    hot, cold = pl.pallas_call(
        functools.partial(kernel, nx, ny, factor, *make_waves(ny)),
        out_shape=(
            jax.ShapeDtypeStruct((HOT, width), f32),
            jax.ShapeDtypeStruct((OWN_ROWS, width), f32),
        ),
        in_specs=[hbm, hbm, hbm, hbm, hbm],
        out_specs=(vmem, vmem),
        scratch_shapes=[
            pltpu.VMEM((look, width), bf16),
            pltpu.VMEM(ids.shape, jnp.int32),
            pltpu.VMEM((look, LANES), i16),
            pltpu.VMEM((look // LANES, 16, LANES), i16),
            pltpu.VMEM((owners, capacity), jnp.int32),
            pltpu.VMEM((owners, -(-cap_pieces // 8) * 8, LANES), jnp.int32),
            pltpu.VMEM((owners, capacity, width), bf16),
            pltpu.VMEM((owners, -(-cap_pieces // 8) * 8, LANES), jnp.int32),
            pltpu.VMEM((2, chain, width), f32),
            pltpu.VMEM((2, chain, width), f32),
            pltpu.VMEM((2, chain, width), f32),
            pltpu.VMEM((nxr - 1, chain // nxr, width), f32),
            pltpu.VMEM((py - 1, chain // py, width), f32),
            pltpu.VMEM((py - 1, chain // nxr // py, width), f32),
            pltpu.VMEM((nxr - 1, chain // nxr // py, width), f32),
            pltpu.VMEM((nyr - 1, piece, width), f32),
            pltpu.VMEM((nyr - 1, piece, width), f32),
            pltpu.VMEM((nx * ny, 2 * piece, width), i16),
            pltpu.VMEM((nx * ny, 1, LANES), f32),
            pltpu.SMEM((owners,), jnp.int32),
            pltpu.SemaphoreType.REGULAR,
            dma((4 + look // KBLOCK,)),
            dma((3 * owners,)),
            dma((3 * owners,)),
            dma((n_sends,)),
            dma((n_sends,)),
        ],
        compiler_params=pltpu.CompilerParams(
            collective_id=0, has_side_effects=True, vmem_limit_bytes=VMEM_KIB * 1024
        ),
    )(*(
        pltpu.with_memory_space_constraint(x, pltpu.HBM)
        for x in (ids, hot_grads, cold_slots.reshape(owners, capacity), cold_counts.reshape(owners), cold_grads.reshape(owners, capacity, width))
    ))
    hot, cold = pl.pallas_call(
        store,
        out_shape=(jax.ShapeDtypeStruct((HOT, width), f32), jax.ShapeDtypeStruct((OWN_ROWS, width), f32)),
        in_specs=[vmem, vmem],
        out_specs=(hbm, hbm),
        scratch_shapes=[dma((2,))],
    )(*(pltpu.with_memory_space_constraint(x, pltpu.VMEM) for x in (hot, cold)))
    return hot, cold.reshape(1, OWN_ROWS, width)


VMEM_KIB = 40000


def solution(mesh):
    body = functools.partial(per_device, mesh.shape["gx"], mesh.shape["gy"])
    return jax.shard_map(
        body,
        mesh=mesh,
        in_specs=(
            P(("gx", "gy")),
            P(("gx", "gy"), None),
            P("gx", "gy", None, None, None),
            P("gx", "gy", None, None),
            P("gx", "gy", None),
        ),
        out_specs=(P(), P("gx", "gy", None)),
        check_vma=False,
    )
```

```python
import functools

import jax
import jax.numpy as jnp
from jax import lax
from jax.experimental import pallas as pl
from jax.experimental.pallas import tpu as pltpu
from jax.sharding import PartitionSpec as P

HOT = 2048
OWN_ROWS = 2048
LANES = 128
HIGH = 4
KBLOCK = 4096
MESH = pl.DeviceIdType.MESH
bf16, f32, i16 = jnp.bfloat16, jnp.float32, jnp.int16


def bits(n):
    assert n & (n - 1) == 0
    return n.bit_length() - 1


def one_hot(row, size):
    places = lax.broadcasted_iota(jnp.int32, (size, LANES), 0).astype(i16)
    return jnp.where(places == jnp.concatenate([row] * (size // 16), axis=0), bf16(1), bf16(0))


def spread(codes, data, wanted):
    return jnp.concatenate(
        [jnp.where(codes == i16(w), data, jnp.zeros_like(data)) for w in wanted], axis=1
    )


def kernel(
    nx, ny, factor, sends, takes,
    ids_ref, hot_ref, slots_ref, counts_ref, cold_ref, hot_out, cold_out,
    hotv, idsv, codes, lows, slotv, sstage, crecv, srecv, tab, give, take,
    l1a, l1b, l2a, l2b, l3a, l3b, coded, scales, counts_smem, fence_sem,
    local_sem, csend, crsem, hsend, hrecv,
):
    gx, gy = lax.axis_index("gx"), lax.axis_index("gy")
    px, py = 2, 2
    nxr, nyr = nx // px, ny // py
    cc, xx = lax.rem(gx, px), gx // px
    yy, zz = lax.rem(gy, py), gy // py
    piece = HOT // (2 * nx * ny)
    chain = HOT // px // 2
    half = chain // 2
    kblocks = hotv.shape[0] // KBLOCK
    cap_pieces = crecv.shape[1] // LANES
    own_low = OWN_ROWS // HIGH

    def at(c, x, y, z):
        return (x * px + c, z * py + y)

    def near_x(j):
        return at(cc, lax.rem(xx + j, nxr), yy, zz)

    def near_y(j):
        return at(cc, xx, lax.rem(yy + j, py), zz)

    def near_z(j):
        return at(cc, xx, yy, lax.rem(zz + j, nyr))

    def plane(dx, dy):
        return at(cc, lax.rem(xx + dx, nxr), lax.rem(yy + dy, py), zz)

    partner = at(1 - cc, xx, yy, zz)

    def cold_peer(t, sign):
        da, db = t // py, t % py
        a = lax.rem(zz + sign * da + nyr, nyr)
        b = lax.rem(yy + sign * db + py, py)
        return a * py + b

    ids_copy = pltpu.make_async_copy(ids_ref, idsv, local_sem.at[0])
    slots_copy = pltpu.make_async_copy(slots_ref, slotv, local_sem.at[1])
    counts_copy = pltpu.make_async_copy(counts_ref, counts_smem, local_sem.at[3])
    own_copy = pltpu.make_async_copy(cold_ref.at[gy], crecv.at[0], local_sem.at[2])
    hot_copies = [
        pltpu.make_async_copy(
            hot_ref.at[pl.ds(k * KBLOCK, KBLOCK), :], hotv.at[pl.ds(k * KBLOCK, KBLOCK), :], local_sem.at[4 + k]
        )
        for k in range(kblocks)
    ]
    barrier = pltpu.get_barrier_semaphore()
    greet = [partner]
    greet += [plane(dx, dy) for dx in range(nxr) for dy in range(py) if dx + dy > 0]
    for t in range(1, ny):
        if t >= py:
            greet.append((gx, cold_peer(t, 1)))
    for device in greet:
        pl.semaphore_signal(barrier, inc=1, device_id=device, device_id_type=MESH)
    counts_copy.start()
    slots_copy.start()
    ids_copy.start()
    for copy in hot_copies:
        copy.start()
    pl.semaphore_wait(barrier, len(greet))

    halves = crecv.shape[1] // 2

    def cold_copy(t, part):
        peer = cold_peer(t, 1)
        if part < 2:
            rows = pl.ds(part * halves, halves)
            source, landing = cold_ref.at[peer, rows, :], crecv.at[t, rows, :]
        else:
            source, landing = sstage.at[peer], srecv.at[t]
        return pltpu.make_async_remote_copy(
            src_ref=source, dst_ref=landing,
            send_sem=csend.at[3 * t + part], recv_sem=crsem.at[3 * t + part],
            device_id=(gx, peer), device_id_type=MESH,
        )

    def cold_start(items):
        for item in items:
            if item % 2 == 0 and item not in sends[0]:
                cold_copy(item // 2, 2).start()
        for item in items:
            cold_copy(item // 2, item % 2).start()

    def fence():
        pl.semaphore_signal(fence_sem, 1)
        pl.semaphore_wait(fence_sem, 1)

    def cold_add(ts, first=False):
        selectors, rows = [], []
        for t in ts:
            slots = sstage[gy] if t == 0 else srecv[t]
            low = jnp.bitwise_and(slots, own_low - 1)
            high = (slots >> bits(own_low)).T
            for j in range(cap_pieces):
                selectors.append(one_hot(jnp.broadcast_to(low[j : j + 1, :], (16, LANES)).astype(i16), own_low))
                code = jnp.broadcast_to(high[:, j : j + 1], (LANES, LANES)).astype(i16)
                rows.append(spread(code, crecv[t, j * LANES : (j + 1) * LANES, :], range(HIGH)))
        total = jnp.dot(
            jnp.concatenate(selectors, axis=1), jnp.concatenate(rows, axis=0), preferred_element_type=f32
        )
        for h in range(HIGH):
            part = total[:, h * LANES : (h + 1) * LANES]
            place = slice(h * own_low, (h + 1) * own_low)
            if first:
                cold_out[place, :] = part
            else:
                cold_out[place, :] += part

    def cold_take(ts):
        for t in ts:
            for part in range(3):
                cold_copy(t, part).wait()
        cold_add(ts)

    def split_ids(ids):
        row = ids & (piece - 1)
        rest = ids >> bits(piece)
        ch = rest & 1
        rest = rest >> 1
        z = ((rest & (nyr - 1)) - zz) & (nyr - 1)
        rest = rest >> bits(nyr)
        y = ((rest & (py - 1)) - yy) & (py - 1)
        rest = rest >> bits(py)
        x = ((rest & (nxr - 1)) - xx) & (nxr - 1)
        core = ((rest >> bits(nxr)) - cc) & 1
        top = jnp.where(ch == 0, x * py + y, y * nxr + x)
        place = (top * nyr + z) * piece + row
        return ch * half + (place & (half - 1)), core * 2 + (place >> bits(half))

    def hot_block(p, k):
        pieces = KBLOCK // LANES
        selectors, rows = [], []
        for q in range(pieces // 8):
            if p == 0:
                low, code = split_ids(idsv[k * pieces // 8 + q])
                columns = code.T
            for j in range(8):
                i = k * pieces + q * 8 + j
                here = slice(i * LANES, (i + 1) * LANES)
                if p == 0:
                    low_row = jnp.broadcast_to(low[j : j + 1, :], (16, LANES)).astype(i16)
                    column = jnp.broadcast_to(columns[:, j : j + 1], (LANES, LANES)).astype(i16)
                    lows[i] = low_row
                    codes[here, :] = column
                else:
                    low_row = lows[i]
                    column = codes[here, :]
                selectors.append(one_hot(low_row, chain))
                rows.append(spread(column, hotv[here, :], (1 - p, 3 - p)))
        total = jnp.dot(
            jnp.concatenate(selectors, axis=1), jnp.concatenate(rows, axis=0), preferred_element_type=f32
        )
        where = slice((1 - p) * half, (2 - p) * half)
        for c in range(2):
            part = total[c * half : (c + 1) * half, :LANES]
            if k == 0:
                tab[c, where, :] = part
            else:
                tab[c, where, :] += part
        if k == 0:
            give[p] = total[:, LANES:]
        else:
            give[p] += total[:, LANES:]

    used = [0]
    sent = []

    def send(src, dst, device):
        copy = pltpu.make_async_remote_copy(
            src_ref=src, dst_ref=dst, send_sem=hsend.at[used[0]], recv_sem=hrecv.at[used[0]],
            device_id=device, device_id_type=MESH,
        )
        used[0] += 1
        copy.start()
        sent.append(copy)
        return copy

    def arrival(ref, index):
        return pltpu.make_async_remote_copy(
            src_ref=ref, dst_ref=ref, send_sem=hsend.at[index], recv_sem=hrecv.at[index],
            device_id=partner, device_id_type=MESH,
        )

    stage1 = [(nxr, near_x, l1a), (py, near_y, l1b)]
    stage2 = [(py, near_y, l2a), (nxr, near_x, l2b)]
    stage3 = [(nyr, near_z, l3a), (nyr, near_z, l3b)]

    def stage1_sends(js):
        copies = {}
        for early in (True, False):
            for c in range(2):
                n, near, landing = stage1[c]
                size = chain // n
                keep = size // stage2[c][0]
                for j in js(n):
                    lo, hi = (keep, size) if early else (0, keep)
                    copies[early, c, j] = send(
                        tab.at[c, pl.ds(j * size + lo, hi - lo), :],
                        landing.at[j - 1, pl.ds(lo, hi - lo), :], near(j),
                    )
        return copies

    def add_take(p):
        where = slice((1 - p) * half, (2 - p) * half)
        for c in range(2):
            tab[c, where, :] += take[p, c * half : (c + 1) * half, :]

    for item in sends[0]:
        cold_copy(item // 2, item % 2).start()
    own_copy.start()
    counts_copy.wait()
    slots_copy.wait()
    owners = slotv.shape[0]
    sub = lax.broadcasted_iota(jnp.int32, (owners, LANES), 0)
    lane = lax.broadcasted_iota(jnp.int32, (owners, LANES), 1)
    count = jnp.zeros((owners, LANES), jnp.int32)
    for o in range(owners):
        count = jnp.where(sub == o, counts_smem[o], count)
    for j in range(sstage.shape[1]):
        if j < cap_pieces:
            sstage[:, j, :] = jnp.where(lane + j * LANES < count, slotv[:, j * LANES : (j + 1) * LANES], -1)
        else:
            sstage[:, j, :] = jnp.full((owners, LANES), -1, jnp.int32)

    for item in sends[0]:
        if item % 2 == 0:
            cold_copy(item // 2, 2).start()
    ids_copy.wait()
    for k in range(kblocks):
        hot_copies[k].wait()
        hot_block(0, k)
    core0 = send(give.at[0], take.at[0], partner)
    cold_start(sends[1])
    fence()
    hot_block(1, 0)
    core0.wait_recv()
    add_take(0)
    first = stage1_sends(lambda n: range(n - 1, n // 2 - 1, -1))
    cold_start(sends[2])
    fence()
    for k in range(1, kblocks):
        hot_block(1, k)
    core1 = send(give.at[1], take.at[1], partner)
    cold_start(sends[3])
    fence()
    own_copy.wait()
    cold_add([0], first=True)
    core1.wait_recv()
    add_take(1)
    first.update(stage1_sends(lambda n: range(n // 2 - 1, 0, -1)))
    second = {}
    for early in (True, False):
        for c in range(2):
            n, _, landing = stage1[c]
            size = chain // n
            keep = size // stage2[c][0]
            lo, hi = (keep, size) if early else (0, keep)
            for j in range(1, n):
                first[early, c, j].wait_recv()
            for j in range(1, n):
                tab[c, lo:hi, :] += landing[j - 1, lo:hi, :]
            if early:
                n2, near, landing2 = stage2[c]
                for j in range(1, n2):
                    second[c, j] = send(tab.at[c, pl.ds(j * keep, keep), :], landing2.at[j - 1], near(j))
    cold_start(sends[4])
    third = {}
    for c in range(2):
        n, _, landing = stage2[c]
        size = chain // stage1[c][0] // n
        for j in range(1, n):
            second[c, j].wait_recv()
        for j in range(1, n):
            tab[c, :size, :] += landing[j - 1]
        n3, near, landing3 = stage3[c]
        for j in range(1, n3):
            third[c, j] = send(tab.at[c, pl.ds(j * piece, piece), :], landing3.at[j - 1], near(j))
    cold_start(sends[5])
    for group in takes[0]:
        cold_take(group)

    def block(c, x, y, z):
        return ((c * nxr + x) * py + y) * nyr + z

    rows = 2 * piece
    groups = rows // 8
    eye = [
        lax.broadcasted_iota(jnp.int32, (8, LANES), 1)
        == lax.broadcasted_iota(jnp.int32, (8, LANES), 0) + g * 8
        for g in range(groups)
    ]
    totals = []
    for c in range(2):
        n3, _, landing3 = stage3[c]
        for j in range(1, n3):
            third[c, j].wait_recv()
        total = tab[c, :piece, :]
        for j in range(1, n3):
            total = total + landing3[j - 1]
        totals.append(total)
    total = jnp.concatenate(totals, axis=0) * factor
    largest = jnp.max(jnp.abs(total), axis=1, keepdims=True)
    unit = jnp.where(largest > 0, 32767.0 / largest, 0.0)
    steps = jnp.round(jnp.clip(total * unit, -32767.0, 32767.0)).astype(jnp.int32).astype(i16)
    mine = block(cc, xx, yy, zz)
    coded[mine] = steps
    size = jnp.broadcast_to(largest * (1.0 / 32767.0), (rows, LANES))
    row = jnp.zeros((8, LANES), f32)
    for g in range(groups):
        row = row + jnp.where(eye[g], size[g * 8 : (g + 1) * 8, :], 0.0)
    scales[mine] = jnp.sum(row, axis=0, keepdims=True)

    def decode(index):
        row = jnp.broadcast_to(scales[index], (8, LANES))
        value = coded[index].astype(jnp.int32).astype(f32)
        for g in range(groups):
            size = jnp.sum(jnp.where(eye[g], row, 0.0), axis=1, keepdims=True)
            hot_out[pl.ds(pl.multiple_of(index * rows + g * 8, 8), 8), :] = value[g * 8 : (g + 1) * 8, :] * size

    def share(place, device):
        index = used[0]
        for ref in (scales, coded):
            send(ref.at[place], ref.at[place], device)
        return index

    def arrived(place, index):
        for n, ref in enumerate((scales, coded)):
            arrival(ref.at[place], index + n).wait_recv()

    z_index = {j: share(mine, near_z(j)) for j in range(1, nyr)}
    plane_steps = [(dx, dy) for dx in range(nxr) for dy in range(py) if dx + dy > 0]
    plane_index, core_index = {}, {}

    def column(c, x, y):
        return pl.ds(block(c, x, y, 0), nyr)

    def from_plane(dx, dy):
        return lax.rem(xx - dx + nxr, nxr), lax.rem(yy - dy + py, py)

    def pass_on(j):
        for dx, dy in plane_steps:
            plane_index[dx, dy, j] = share(block(cc, xx, yy, lax.rem(zz + j, nyr)), plane(dx, dy))

    cold_start(sends[6])
    pass_on(0)
    cold_start(sends[7])
    order = sorted(range(1, nyr), key=lambda j: min(j, nyr - j))
    for j in order:
        arrived(block(cc, xx, yy, lax.rem(zz + j, nyr)), z_index[nyr - j])
        pass_on(j)
    core_index[0, 0] = share(column(cc, xx, yy), partner)
    cold_start(sends[8])
    for group in takes[1]:
        cold_take(group)
    for j in [0] + order:
        decode(block(cc, xx, yy, lax.rem(zz + j, nyr)))
    for dx, dy in plane_steps:
        x, y = from_plane(dx, dy)
        for j in [0] + order:
            arrived(block(cc, x, y, lax.rem(zz + j, nyr)), plane_index[dx, dy, j])
        core_index[dx, dy] = share(column(cc, x, y), partner)
        for z in range(nyr):
            decode(block(cc, x, y, z))
    for group in takes[2][:-1]:
        cold_take(group)
    for (dx, dy), index in core_index.items():
        x, y = from_plane(dx, dy)
        arrived(column(1 - cc, x, y), index)
        for z in range(nyr):
            decode(block(1 - cc, x, y, z))
    cold_take(takes[2][-1])
    for copy in sent:
        copy.wait_send()


def store(hot_ref, cold_ref, hot_out, cold_out, sem):
    copies = [
        pltpu.make_async_copy(hot_ref, hot_out, sem.at[0]),
        pltpu.make_async_copy(cold_ref, cold_out, sem.at[1]),
    ]
    for copy in copies:
        copy.start()
    for copy in copies:
        copy.wait()


def make_waves(ny):
    if ny == 8:
        return SENDS, TAKES
    every = list(range(1, ny))
    early, late = every[: ny // 2], every[ny // 2 :]
    both = lambda ts: [2 * t + h for t in ts for h in range(2)]
    return [both(early), [], [], [], [], [], [], both(late), []], [[[t] for t in early], [], [[t] for t in late]]


SENDS = [[6, 7, 2, 3, 10, 11], [], [], [8, 9], [], [], [4, 12], [5, 13, 14, 15], []]
TAKES = [[[3, 1]], [[5, 4]], [[2, 6], [7]]]


def per_device(nx, ny, hot_ids, hot_grads, cold_grads, cold_slots, cold_counts):
    look, width = hot_grads.shape
    owners, capacity = cold_slots.shape[2], cold_slots.shape[3]
    px, py = 2, 2
    nxr, nyr = nx // px, ny // py
    factor = (HOT / (look * nx * ny)) ** 0.5
    chain = HOT // px // 2
    piece = chain // (nxr * ny)
    cap_pieces = capacity // LANES
    ids = hot_ids.reshape(-1, 8, LANES)
    n_sends = 2 + 3 * (nxr - 1) + 3 * (py - 1) + 4 * (nyr - 1) + 2 * (nxr * py - 1) * nyr + 2 * nxr * py
    hbm = pl.BlockSpec(memory_space=pltpu.HBM)
    vmem = pl.BlockSpec(memory_space=pltpu.VMEM)
    dma = pltpu.SemaphoreType.DMA
    hot, cold = pl.pallas_call(
        functools.partial(kernel, nx, ny, factor, *make_waves(ny)),
        out_shape=(
            jax.ShapeDtypeStruct((HOT, width), f32),
            jax.ShapeDtypeStruct((OWN_ROWS, width), f32),
        ),
        in_specs=[hbm, hbm, hbm, hbm, hbm],
        out_specs=(vmem, vmem),
        scratch_shapes=[
            pltpu.VMEM((look, width), bf16),
            pltpu.VMEM(ids.shape, jnp.int32),
            pltpu.VMEM((look, LANES), i16),
            pltpu.VMEM((look // LANES, 16, LANES), i16),
            pltpu.VMEM((owners, capacity), jnp.int32),
            pltpu.VMEM((owners, -(-cap_pieces // 8) * 8, LANES), jnp.int32),
            pltpu.VMEM((owners, capacity, width), bf16),
            pltpu.VMEM((owners, -(-cap_pieces // 8) * 8, LANES), jnp.int32),
            pltpu.VMEM((2, chain, width), f32),
            pltpu.VMEM((2, chain, width), f32),
            pltpu.VMEM((2, chain, width), f32),
            pltpu.VMEM((nxr - 1, chain // nxr, width), f32),
            pltpu.VMEM((py - 1, chain // py, width), f32),
            pltpu.VMEM((py - 1, chain // nxr // py, width), f32),
            pltpu.VMEM((nxr - 1, chain // nxr // py, width), f32),
            pltpu.VMEM((nyr - 1, piece, width), f32),
            pltpu.VMEM((nyr - 1, piece, width), f32),
            pltpu.VMEM((nx * ny, 2 * piece, width), i16),
            pltpu.VMEM((nx * ny, 1, LANES), f32),
            pltpu.SMEM((owners,), jnp.int32),
            pltpu.SemaphoreType.REGULAR,
            dma((4 + look // KBLOCK,)),
            dma((3 * owners,)),
            dma((3 * owners,)),
            dma((n_sends,)),
            dma((n_sends,)),
        ],
        compiler_params=pltpu.CompilerParams(
            collective_id=0, has_side_effects=True, vmem_limit_bytes=VMEM_KIB * 1024
        ),
    )(*(
        pltpu.with_memory_space_constraint(x, pltpu.HBM)
        for x in (ids, hot_grads, cold_slots.reshape(owners, capacity), cold_counts.reshape(owners), cold_grads.reshape(owners, capacity, width))
    ))
    hot, cold = pl.pallas_call(
        store,
        out_shape=(jax.ShapeDtypeStruct((HOT, width), f32), jax.ShapeDtypeStruct((OWN_ROWS, width), f32)),
        in_specs=[vmem, vmem],
        out_specs=(hbm, hbm),
        scratch_shapes=[dma((2,))],
    )(*(pltpu.with_memory_space_constraint(x, pltpu.VMEM) for x in (hot, cold)))
    return hot, cold.reshape(1, OWN_ROWS, width)


VMEM_KIB = 40000


def solution(mesh):
    body = functools.partial(per_device, mesh.shape["gx"], mesh.shape["gy"])
    return jax.shard_map(
        body,
        mesh=mesh,
        in_specs=(
            P(("gx", "gy")),
            P(("gx", "gy"), None),
            P("gx", "gy", None, None, None),
            P("gx", "gy", None, None),
            P("gx", "gy", None),
        ),
        out_specs=(P(), P("gx", "gy", None)),
        check_vma=False,
    )
```
